32 devices in a mesh: dp: 4 (over y, core), mp: 8 (over z, x).
Axes of the slice: x: 2, y: 2, z: 4, core: 2. Of those that a mesh axis runs over, the one named last changes fastest.
Arguments:
- table: bfloat16 [16384, 1024], P('mp'), may hold values from -200 to 200
- triples: int32 [32, 3], P('dp'), may hold values from 0 to 16383
- words: int32 [32, 61], P('dp'), may hold values from 0 to 16383
- labels: int32 [32], P('dp'), may hold values 0 or 1
- in_gain: float32 [1024], replicated, may hold values from 0.5 to 1.5
- up_weight: bfloat16 [1024, 4096], P(None, 'mp'), may hold values from -0.1875 to 0.1875
- down_weight: bfloat16 [4096, 1024], P('mp'), may hold values from -0.09375 to 0.09375
- out_gain: float32 [1024], P('mp'), may hold values from 0.5 to 1.5
- class_weight: float32 [1024], P('mp'), may hold values from -6 to 6
Outputs:
- encoded: bfloat16 [2048, 1024], P('dp', 'mp')
- scores: float32 [32], P('dp')
- class_grad: float32 [1024], P('mp')
The draws below stay inside these ranges and needn't reach their ends.
All inputs are finite; a program needn't handle non-finite values. No bound on the sum of `labels` on one device may be relied on, other than what follows from the above.
Results may differ from the reference program's by a relative error of at most 0.0075.
Values may be sent and summed in bfloat16 or wider, within the bound.
A program may use at most 64 MiB of HBM per device.

```python
import jax
import jax.numpy as jnp
from jax import lax

D = 1024
FF = 4096
SEQ = 64
WORDS = 61
ENTITIES = 16384
TRIPLES = 32


def draw_table(key, part):
    first = jax.random.fold_in(key, 0)
    base = jnp.clip(jax.random.normal(first, (ENTITIES, D), jnp.float32), -6.0, 6.0)
    column_scale = jnp.exp(jnp.log(3.0) * jnp.arange(D, dtype=jnp.float32) / D)
    return (base * column_scale[None, :]).astype(jnp.bfloat16)


def plant(entries, own_key, low, top_value):
    longest = entries.shape.index(max(entries.shape))
    spots = []
    for shift in (0, 1):
        where = [jax.random.randint(jax.random.fold_in(own_key, axis), (), 0, length) for axis, length in enumerate(entries.shape)]
        where[longest] = (where[longest] + shift) % entries.shape[longest]
        spots.append(tuple(where))
    return entries.at[spots[0]].set(low).at[spots[1]].set(top_value)


def levels(key, extent, cuts, least, top_value):
    factor_of = 1.0
    for dim, blocks in cuts:
        heights = jax.random.uniform(jax.random.fold_in(jax.random.fold_in(key, 6), dim), (blocks,), jnp.float32, least / len(cuts), top_value / len(cuts))
        factor_of = factor_of * jnp.repeat(jnp.exp(heights), extent[dim] // blocks).reshape((-1,) + (1,) * (len(extent) - 1 - dim))
    return factor_of


def gaussian(key, dims, scale, limit, shards=(), held_as=jnp.bfloat16):
    level = levels(key, dims, shards, -0.22, 0.18) if shards else 1.0
    drawn = jax.random.normal(key, dims, jnp.float32) * scale * level
    return jnp.minimum(jnp.maximum(drawn, -limit), limit).astype(held_as)


def setup_inputs(seed: int = 0) -> dict:
    seeds = jax.random.split(jax.random.key(seed), 10)
    table = draw_table(jax.random.fold_in(seeds[9], 71), 0)
    triples = plant(jax.random.randint(seeds[1], (TRIPLES, 3), 0, ENTITIES), jax.random.fold_in(seeds[1], 1), 0, ENTITIES - 1).astype(jnp.int32)
    words = plant(jax.random.randint(seeds[2], (TRIPLES, WORDS), 0, ENTITIES), jax.random.fold_in(seeds[2], 1), 0, ENTITIES - 1).astype(jnp.int32)
    labels = plant((jax.random.randint(seeds[3], (TRIPLES,), 0, 2) < 1).astype(jnp.int32), jax.random.fold_in(seeds[3], 1), 0, 1)
    in_gain = jnp.clip(1.0 + 0.1 * jax.random.normal(seeds[4], (D,), jnp.float32), 0.5, 1.5)
    up_weight = gaussian(seeds[5], (D, FF), D ** -0.5, 0.1875, ((1, 8),))
    down_weight = gaussian(seeds[6], (FF, D), FF ** -0.5, 0.09375, ((0, 8),))
    out_gain = jnp.clip(1.0 + 0.1 * jax.random.normal(seeds[7], (D,), jnp.float32), 0.5, 1.5)
    class_weight = gaussian(seeds[8], (D,), 1.0, 6.0, ((0, 8),), jnp.float32)
    return dict(table=table, triples=triples, words=words, labels=labels, in_gain=in_gain, up_weight=up_weight, down_weight=down_weight, out_gain=out_gain, class_weight=class_weight)


def norm_rows(values, gain):
    width = values.shape[1]
    mean = lax.optimization_barrier(jnp.sum(values, axis=1)) / width
    var = lax.optimization_barrier(jnp.sum(values * values, axis=1)) / width - mean * mean
    return (values - mean[:, None]) * lax.rsqrt(var + 1e-05)[:, None] * gain

def reference(table, triples, words, labels, in_gain, up_weight, down_weight, out_gain, class_weight):
    ids = jnp.concatenate([triples, words], axis=1).reshape(-1).astype(jnp.int32)
    embed = table[ids].astype(jnp.float32)
    normed = norm_rows(embed, in_gain).astype(jnp.bfloat16)
    hidden = jnp.dot(normed, up_weight, preferred_element_type=jnp.float32)
    active = jax.nn.gelu(hidden, approximate=False).astype(jnp.bfloat16)
    mixed = jnp.dot(active, down_weight, preferred_element_type=jnp.float32)
    resid = normed.astype(jnp.float32) + mixed
    encoded = norm_rows(resid, out_gain).astype(jnp.bfloat16)
    pooled = lax.optimization_barrier(jnp.mean(encoded.astype(jnp.float32).reshape(TRIPLES, SEQ, D), axis=1))
    scores = jnp.dot(pooled, class_weight, precision=lax.Precision.HIGHEST)
    diff = jax.nn.sigmoid(scores) - labels.astype(jnp.float32)
    class_grad = jnp.dot(diff, pooled, precision=lax.Precision.HIGHEST)
    return (encoded, scores, class_grad)
```

```python
import functools
import math

import jax
import jax.numpy as jnp
from jax import lax
from jax.experimental import pallas as pl
from jax.experimental.pallas import tpu as pltpu
from jax.sharding import PartitionSpec as P

MESH = pl.DeviceIdType.MESH
BF16 = jnp.bfloat16
F32 = jnp.float32


def each(count, body):
    if count <= 8:
        for k in range(count):
            body(k)
    else:
        lax.fori_loop(0, count, lambda k, c: (body(k), c)[1], 0)


def norm_rows(values, gain, width):
    mean = jnp.sum(values, axis=1, keepdims=True) / width
    var = jnp.sum(values * values, axis=1, keepdims=True) / width - mean * mean
    return ((values - mean) * lax.rsqrt(var + 1e-05) * gain).astype(BF16)


def kernel(
    n, ndp, seq,
    ids, table, up, down, in_gain, out_gain, class_w, labels,
    enc_out, score_out, grad_out,
    tab_v, up_v, down_v, a_send, a_recv, b_send, b_recv, gath, c_send, c_recv, part,
    d_send, d_recv, og_all, cw_all, e_send, e_recv, s_send, s_recv, q_send, q_recv,
    loc_sem, a_ss, a_rs, b_ss, b_rs, gz_ss, gx_ss, g_rs, c_ss, c_rs, d_ss, d_rs,
    w_ss, w_rs, e_ss, e_rs, s_ss, s_rs, q_ss, q_rs,
):
    Z = n // 2
    me = lax.axis_index("mp")
    dme = lax.axis_index("dp")
    z, x = me // 2, me % 2
    ox = 1 - x
    partner = z * 2 + ox
    tok = ids.shape[1]
    width = table.shape[1]
    entries = table.shape[0]
    feat = enc_out.shape[2]
    triples = labels.shape[0]

    def remote(src, dst, ss, rs, mp=None, dp=None):
        where = {"mp": mp} if dp is None else {"dp": dp}
        return pltpu.make_async_remote_copy(
            src_ref=src, dst_ref=dst, send_sem=ss, recv_sem=rs, device_id=where, device_id_type=MESH
        )

    loads = [
        pltpu.make_async_copy(src, dst, loc_sem.at[i])
        for i, (src, dst) in enumerate(((table, tab_v), (up, up_v), (down, down_v)))
    ]
    for copy in loads:
        copy.start()

    barrier = pltpu.get_barrier_semaphore()

    def greet(j):
        pl.semaphore_signal(barrier, inc=1, device_id={"mp": (me + 1 + j) % n}, device_id_type=MESH)

    each(n - 1, greet)
    for j in range(1, ndp):
        pl.semaphore_signal(barrier, inc=1, device_id={"dp": (dme + j) % ndp}, device_id_type=MESH)

    loads[0].wait()

    def half(side):
        local = jnp.concatenate([ids[zk * 2 + side] for zk in range(Z)], axis=0) - me * entries
        lanes = lax.broadcasted_iota(jnp.int32, (local.shape[0], entries), 1)
        hot = jnp.where(lanes == local, 1.0, 0.0).astype(BF16)
        embed = jnp.dot(hot, tab_v[...], preferred_element_type=F32)
        return norm_rows(embed, in_gain[...], width)

    rows = half(ox)
    for zk in range(Z):
        a_send[zk] = rows[zk * tok:(zk + 1) * tok]
    pl.semaphore_wait(barrier, n - 1 + ndp - 1)

    def a_copy(zk):
        return remote(a_send.at[zk], a_recv.at[zk], a_ss.at[zk], a_rs.at[zk], mp=partner)

    each(Z, lambda k: a_copy((z + 1 + k) % Z).start())

    def w_copies(j):
        p = (me + 1 + j) % n
        return (
            remote(out_gain, og_all.at[me], w_ss.at[0, p], w_rs.at[0, me], mp=p),
            remote(class_w, cw_all.at[me], w_ss.at[1, p], w_rs.at[1, me], mp=p),
        )

    def w_start(j):
        for copy in w_copies(j):
            copy.start()

    each(n - 1, w_start)
    og_all[me] = out_gain[...]
    cw_all[me] = class_w[...]

    rows = half(x)
    for zk in range(Z):
        b_send[zk] = rows[zk * tok:(zk + 1) * tok]

    def b_copy(zk):
        return remote(b_send.at[zk], b_recv.at[z], b_ss.at[zk], b_rs.at[z], mp=zk * 2 + x)

    def b_step(k):
        zk = (z + 1 + k) % Z
        a_copy(zk).wait_recv()
        b_send[zk] = b_send[zk] + a_recv[zk]
        if isinstance(k, int) and k == Z - 1:
            return
        b_copy(zk).start()

    each(Z - 1, b_step)
    b_step(Z - 1)

    def from_z(k):
        return (z + Z - 1 - k) % Z

    def b_in(zs):
        return remote(b_send.at[z], b_recv.at[zs], b_ss.at[z], b_rs.at[zs], mp=me)

    each(Z - 1, lambda k: b_in(from_z(k)).wait_recv())
    total = b_send[z]
    if Z <= 8:
        for k in range(Z - 1):
            total = total + b_recv[from_z(k)]
    else:
        total = lax.fori_loop(0, Z - 1, lambda k, t: t + b_recv[from_z(k)], total)
    gath[me] = total

    def gz_copy(zk):
        return remote(gath.at[me], gath.at[me], gz_ss.at[zk], g_rs.at[me], mp=zk * 2 + x)

    def gx_copy(zk):
        b = zk * 2 + x
        return remote(gath.at[b], gath.at[b], gx_ss.at[zk], g_rs.at[b], mp=partner)

    def g_in(b):
        return remote(gath.at[b], gath.at[b], gz_ss.at[z], g_rs.at[b], mp=me)

    gx_copy(z).start()
    each(Z - 1, lambda k: gz_copy((z + 1 + k) % Z).start())
    loads[1].wait()
    loads[2].wait()

    def c_copy(zk):
        return remote(c_send.at[zk], c_recv.at[zk], c_ss.at[zk], c_rs.at[zk], mp=partner)

    def d_copy(zk):
        return remote(d_send.at[zk], d_recv.at[z], d_ss.at[zk], d_rs.at[z], mp=zk * 2 + x)

    def ffn(zs, own):
        if not own:
            g_in(zs * 2 + x).wait_recv()
            gx_copy(zs).start()
        g_in(zs * 2 + ox).wait_recv()
        both = jnp.concatenate([gath[zs * 2 + ox], gath[zs * 2 + x]], axis=0)
        hidden = jnp.dot(both, up_v[...], preferred_element_type=F32)
        active = (0.5 * hidden * (1.0 + lax.erf(hidden * (1.0 / math.sqrt(2.0))))).astype(BF16)
        terms = jnp.dot(active, down_v[...], preferred_element_type=F32)
        c_send[zs] = terms[:tok].astype(BF16)
        c_copy(zs).start()
        part[zs] = terms[tok:]

    def pass_on(zs):
        c_copy(zs).wait_recv()
        d_send[zs] = (part[zs] + c_recv[zs].astype(F32)).astype(BF16)
        d_copy(zs).start()

    ffn(z, True)

    def step(k):
        ffn(from_z(k), False)
        if isinstance(k, int):
            if k > 0:
                pass_on(from_z(k - 1))
        else:
            pl.when(k > 0)(lambda: pass_on(from_z(k - 1)))

    each(Z - 1, step)
    pass_on(from_z(Z - 2))

    c_copy(z).wait_recv()
    mixed = part[z] + c_recv[z].astype(F32)

    def d_in(zs):
        return remote(d_send.at[z], d_recv.at[zs], d_ss.at[z], d_rs.at[zs], mp=me)

    each(Z - 1, lambda k: d_in(from_z(k)).wait_recv())
    if Z <= 8:
        for k in range(Z - 1):
            mixed = mixed + d_recv[from_z(k)].astype(F32)
    else:
        mixed = lax.fori_loop(0, Z - 1, lambda k, t: t + d_recv[from_z(k)].astype(F32), mixed)
    resid = gath[me].astype(F32) + mixed

    def w_in(j):
        src = (me + n - 1 - j) % n
        for i, (ref, dst) in enumerate(((out_gain, og_all), (class_w, cw_all))):
            remote(ref, dst.at[src], w_ss.at[i, me], w_rs.at[i, src], mp=me).wait_recv()

    each(n - 1, w_in)
    gain = jnp.concatenate([og_all[p] for p in range(n)], axis=1)
    weight = jnp.concatenate([cw_all[p] for p in range(n)], axis=1)
    encoded = norm_rows(resid, gain, width)
    for p in range(n):
        e_send[p] = encoded[:, p * feat:(p + 1) * feat]
    score = jnp.sum(encoded.astype(F32) * weight) / seq
    s_send[...] = jnp.full(s_send.shape, score, F32)

    def e_copies(j):
        p = (me + 1 + j) % n
        return (
            remote(e_send.at[p], e_recv.at[me], e_ss.at[p], e_rs.at[me], mp=p),
            remote(s_send, s_recv.at[me], s_ss.at[p], s_rs.at[me], mp=p),
        )

    def e_start(j):
        for copy in e_copies(j):
            copy.start()

    each(n - 1, e_start)
    e_recv[me] = e_send[me]
    s_recv[me] = s_send[...]

    def e_in(j):
        src = (me + n - 1 - j) % n
        remote(e_send.at[me], e_recv.at[src], e_ss.at[me], e_rs.at[src], mp=me).wait_recv()
        remote(s_send, s_recv.at[src], s_ss.at[me], s_rs.at[src], mp=me).wait_recv()

    each(n - 1, e_in)
    per = n // triples
    lane = lax.broadcasted_iota(jnp.int32, (1, triples), 1)
    scores = jnp.zeros((1, triples), F32)
    grad = jnp.zeros((1, feat), F32)
    for t in range(triples):
        logit = s_recv[t * per]
        block = jnp.sum(e_recv[t * per].astype(F32), axis=0, keepdims=True)
        for p in range(t * per + 1, (t + 1) * per):
            logit = logit + s_recv[p]
            block = block + jnp.sum(e_recv[p].astype(F32), axis=0, keepdims=True)
        scores = jnp.where(lane == t, logit[0:1, :triples], scores)
        diff = jax.nn.sigmoid(logit[0:1, :feat]) - labels[t].astype(F32)
        grad = grad + diff * (block / seq)
    q_send[...] = grad

    def q_copy(j):
        return remote(
            q_send, q_recv.at[dme], q_ss.at[j], q_rs.at[dme], dp=(dme + j) % ndp
        )

    for j in range(1, ndp):
        q_copy(j).start()
    score_out[...] = scores
    enc_out[...] = e_recv[...]

    each(Z, lambda k: a_copy((z + 1 + k) % Z).wait_send())
    each(Z - 1, lambda k: b_copy((z + 1 + k) % Z).wait_send())
    each(Z - 1, lambda k: gz_copy((z + 1 + k) % Z).wait_send())
    each(Z, lambda k: gx_copy((z + 1 + k) % Z).wait_send())
    each(Z, lambda k: c_copy((z + 1 + k) % Z).wait_send())
    each(Z - 1, lambda k: d_copy((z + 1 + k) % Z).wait_send())

    def ends(j):
        for copy in w_copies(j) + e_copies(j):
            copy.wait_send()

    each(n - 1, ends)
    for j in range(1, ndp):
        src = (dme + ndp - j) % ndp
        remote(q_send, q_recv.at[src], q_ss.at[j], q_rs.at[src], dp=dme).wait_recv()
        grad = grad + q_recv[src]
        q_copy(j).wait_send()
    grad_out[...] = grad


def on_device(
    n, ndp, table, triples, words, labels, in_gain, up_weight, down_weight, out_gain, class_weight
):
    ids = jnp.concatenate([triples, words], axis=1)
    seq = ids.shape[1]
    rows = ids.size
    tok = rows // n
    entries, width = table.shape
    units = up_weight.shape[1]
    feat = width // n
    Z = n // 2
    T = triples.shape[0]
    dma = pltpu.SemaphoreType.DMA
    vm = pl.BlockSpec(memory_space=pltpu.VMEM)
    hbm = pl.BlockSpec(memory_space=pl.ANY)
    zblk = pltpu.VMEM((Z, tok, width), BF16)
    wide = max(128, feat)
    enc, scores, grad = pl.pallas_call(
        functools.partial(kernel, n, ndp, seq),
        out_shape=(
            jax.ShapeDtypeStruct((n, tok, feat), BF16),
            jax.ShapeDtypeStruct((1, T), F32),
            jax.ShapeDtypeStruct((1, feat), F32),
        ),
        in_specs=[vm, hbm, hbm, hbm, vm, vm, vm, pl.BlockSpec(memory_space=pltpu.SMEM)],
        out_specs=(vm, vm, vm),
        scratch_shapes=[
            pltpu.VMEM((entries, width), BF16),
            pltpu.VMEM((width, units), BF16),
            pltpu.VMEM((units, width), BF16),
            zblk, zblk, zblk, zblk,
            pltpu.VMEM((n, tok, width), BF16),
            zblk, zblk,
            pltpu.VMEM((Z, tok, width), F32),
            zblk, zblk,
            pltpu.VMEM((n, 1, feat), F32),
            pltpu.VMEM((n, 1, feat), F32),
            pltpu.VMEM((n, tok, feat), BF16),
            pltpu.VMEM((n, tok, feat), BF16),
            pltpu.VMEM((8, wide), F32),
            pltpu.VMEM((n, 8, wide), F32),
            pltpu.VMEM((1, feat), F32),
            pltpu.VMEM((ndp, 1, feat), F32),
            dma((3,)),
            dma((Z,)), dma((Z,)), dma((Z,)), dma((Z,)),
            dma((Z,)), dma((Z,)), dma((n,)),
            dma((Z,)), dma((Z,)), dma((Z,)), dma((Z,)),
            dma((2, n)), dma((2, n)),
            dma((n,)), dma((n,)), dma((n,)), dma((n,)),
            dma((ndp,)), dma((ndp,)),
        ],
        compiler_params=pltpu.CompilerParams(
            collective_id=0, has_side_effects=True, vmem_limit_bytes=48 * 1024 * 1024
        ),
    )(
        ids.reshape(n, tok, 1), table, up_weight, down_weight, in_gain.reshape(1, -1),
        out_gain.reshape(1, -1), class_weight.reshape(1, -1), labels,
    )
    return enc.reshape(rows, feat), scores.reshape(-1), grad.reshape(-1)


def solution(mesh):
    return jax.shard_map(
        functools.partial(on_device, mesh.shape["mp"], mesh.shape["dp"]),
        mesh=mesh,
        in_specs=(
            P("mp", None), P("dp", None), P("dp", None), P("dp"), P(),
            P(None, "mp"), P("mp", None), P("mp"), P("mp"),
        ),
        out_specs=(P("dp", "mp"), P("dp"), P("mp")),
        check_vma=False,
    )
```

```python
import functools
import math

import jax
import jax.numpy as jnp
from jax import lax
from jax.experimental import pallas as pl
from jax.experimental.pallas import tpu as pltpu
from jax.sharding import PartitionSpec as P

MESH = pl.DeviceIdType.MESH
BF16 = jnp.bfloat16
F32 = jnp.float32


def each(count, body):
    if count <= 8:
        for k in range(count):
            body(k)
    else:
        lax.fori_loop(0, count, lambda k, c: (body(k), c)[1], 0)


def norm_rows(values, gain, width):
    mean = jnp.sum(values, axis=1, keepdims=True) / width
    var = jnp.sum(values * values, axis=1, keepdims=True) / width - mean * mean
    return ((values - mean) * lax.rsqrt(var + 1e-05) * gain).astype(BF16)


def kernel(
    n, ndp, seq,
    ids, table, up, down, in_gain, out_gain, class_w, labels,
    enc_out, score_out, grad_out,
    tab_v, up_v, down_v, upx_v, downx_v, a_send, a_recv, own, sw_send, sw_recv,
    rows_v, terms_v, keep, part, d_send, d_recv,
    og_all, cw_all, e_send, e_recv, s_send, s_recv, q_send, q_recv,
    loc_sem, wx_ss, wx_rs, wy_ss, wy_rs, wc_ss, wc_rs, a_ss, a_rs, sw_ss, sw_rs, d_ss, d_rs,
    w_ss, w_rs, e_ss, e_rs, s_ss, s_rs, q_ss, q_rs,
):
    Z = n // 2
    me = lax.axis_index("mp")
    dme = lax.axis_index("dp")
    z, x = me // 2, me % 2
    ox = 1 - x
    partner = z * 2 + ox
    across = (dme + ndp // 2) % ndp
    beside = dme // 2 * 2 + 1 - dme % 2
    chunks, chunk_rows, width = own.shape
    r = chunk_rows // Z
    entries = table.shape[0]
    units = up.shape[1]
    feat = enc_out.shape[2]
    triples = labels.shape[0]

    def remote(src, dst, ss, rs, mp=None, dp=None):
        where = {"mp": mp} if dp is None else {"dp": dp}
        return pltpu.make_async_remote_copy(
            src_ref=src, dst_ref=dst, send_sem=ss, recv_sem=rs, device_id=where, device_id_type=MESH
        )

    loads = [
        pltpu.make_async_copy(src, dst, loc_sem.at[i])
        for i, (src, dst) in enumerate(((table, tab_v), (up, up_v), (down, down_v)))
    ]
    for copy in loads:
        copy.start()

    barrier = pltpu.get_barrier_semaphore()

    def greet(j):
        pl.semaphore_signal(barrier, inc=1, device_id={"mp": (me + 1 + j) % n}, device_id_type=MESH)

    each(n - 1, greet)
    for j in range(1, ndp):
        pl.semaphore_signal(barrier, inc=1, device_id={"dp": (dme + j) % ndp}, device_id_type=MESH)
    pl.semaphore_wait(barrier, n - 1 + ndp - 1)

    def quarter(ref, d):
        size = ref.shape[0] // ndp
        return ref.at[pl.ds(pl.multiple_of(d * size, size), size)]

    pairs = ((up, upx_v), (down, downx_v))

    def wx_copy(i):
        src, dst = pairs[i]
        return remote(quarter(src, dme), quarter(dst, dme), wx_ss.at[i], wx_rs.at[i], mp=partner)

    def wy_copy(i, d):
        ref = pairs[i][1]
        return remote(quarter(ref, d), quarter(ref, d), wy_ss.at[i], wy_rs.at[i], dp=across)

    def wc_copy(i, d, k):
        ref = pairs[i][1]
        return remote(quarter(ref, d), quarter(ref, d), wc_ss.at[i, k], wc_rs.at[i, k], dp=beside)

    wx_copy(0).start()
    wx_copy(1).start()

    def w_copies(j):
        p = (me + 1 + j) % n
        return (
            remote(out_gain, og_all.at[me], w_ss.at[0, p], w_rs.at[0, me], mp=p),
            remote(class_w, cw_all.at[me], w_ss.at[1, p], w_rs.at[1, me], mp=p),
        )

    def w_start(j):
        for copy in w_copies(j):
            copy.start()

    each(n - 1, w_start)
    og_all[me] = out_gain[...]
    cw_all[me] = class_w[...]
    loads[0].wait()

    def half(side):
        local = ids[side] - me * entries
        lanes = lax.broadcasted_iota(jnp.int32, (local.shape[0], entries), 1)
        hot = jnp.where(lanes == local, 1.0, 0.0).astype(BF16)
        embed = jnp.dot(hot, tab_v[...], preferred_element_type=F32)
        return norm_rows(embed, in_gain[...], width)

    def a_copy(j):
        return remote(a_send.at[j], a_recv.at[j], a_ss.at[j], a_rs.at[j], mp=partner)

    rows = half(ox)
    for j in range(chunks):
        a_send[j] = rows[j * chunk_rows:(j + 1) * chunk_rows]
        a_copy(j).start()
    rows = half(x)
    for j in range(chunks):
        own[j] = rows[j * chunk_rows:(j + 1) * chunk_rows]

    for i in range(2):
        wx_copy(i).wait_recv()
        wy_copy(i, dme).start()
        wc_copy(i, dme, 0).start()

    first = z // (Z // 2)
    second = 1 - first
    edge = jnp.logical_or(z == 0, z == Z - 1)
    inner = jnp.logical_not(edge)

    def sweep(way, j):
        return remote(
            sw_send.at[way, j], sw_recv.at[way, j], sw_ss.at[way, j], sw_rs.at[way, j],
            mp=(z + 1 - 2 * way) * 2 + x,
        )

    def sweep_in(way, j):
        return remote(
            sw_send.at[way, j], sw_recv.at[way, j], sw_ss.at[way, j], sw_rs.at[way, j], mp=me
        )

    def arrive(j):
        a_copy(j).wait_recv()
        own[j] = own[j] + a_recv[j]

        @pl.when(edge)
        def _():
            sw_recv[first, j] = jnp.zeros((chunk_rows, width), BF16)

        @pl.when(inner)
        def _():
            sweep_in(first, j).wait_recv()

        sw_send[first, j] = own[j] + sw_recv[first, j]
        sweep(first, j).start()

    def d_copy(j, zk):
        return remote(
            d_send.at[j, zk], d_recv.at[j, z], d_ss.at[j, zk], d_rs.at[j, z], mp=zk * 2 + x
        )

    def act(hidden):
        return (0.5 * hidden * (1.0 + lax.erf(hidden * (1.0 / math.sqrt(2.0))))).astype(BF16)

    def finish(j):
        sweep_in(second, j).wait_recv()

        @pl.when(inner)
        def _():
            sw_send[second, j] = own[j] + sw_recv[second, j]
            sweep(second, j).start()

        full = own[j] + sw_recv[0, j] + sw_recv[1, j]
        for zk in range(Z):
            rows_v[zk] = full[zk * r:(zk + 1) * r]
        keep[j] = rows_v[z].astype(F32)
        if j == 0:
            for i in range(2):
                wc_copy(i, beside, 0).wait_recv()
                wc_copy(i, (beside + ndp // 2) % ndp, 1).wait_recv()
            loads[1].wait()
            loads[2].wait()
        mine = act(jnp.dot(full, up_v[...], preferred_element_type=F32))
        theirs = act(jnp.dot(full, upx_v[...], preferred_element_type=F32))
        terms = jnp.dot(mine, down_v[...], preferred_element_type=F32)
        terms = terms + jnp.dot(theirs, downx_v[...], preferred_element_type=F32)
        for zk in range(Z):
            terms_v[zk] = terms[zk * r:(zk + 1) * r]
            d_send[j, zk] = terms[zk * r:(zk + 1) * r].astype(BF16)
        each(Z - 1, lambda k: d_copy(j, (z + 1 + k) % Z).start())
        part[j] = terms_v[z]

    lag = min(2, chunks)
    for t in range(chunks + lag):
        if t < chunks:
            arrive(t)
        if t == 0:
            for i in range(2):
                wy_copy(i, across).wait_recv()
                wc_copy(i, across, 1).start()
        if t >= lag:
            finish(t - lag)

    def w_in(j):
        src = (me + n - 1 - j) % n
        for i, (ref, dst) in enumerate(((out_gain, og_all), (class_w, cw_all))):
            remote(ref, dst.at[src], w_ss.at[i, me], w_rs.at[i, src], mp=me).wait_recv()

    each(n - 1, w_in)
    gain = jnp.concatenate([og_all[p] for p in range(n)], axis=1)
    weight = jnp.concatenate([cw_all[p] for p in range(n)], axis=1)

    def d_in(j, zs):
        return remote(d_send.at[j, z], d_recv.at[j, zs], d_ss.at[j, z], d_rs.at[j, zs], mp=me)

    score = jnp.zeros((), F32)
    for j in range(chunks):
        each(Z - 1, lambda k: d_in(j, (z + 1 + k) % Z).wait_recv())
        resid = keep[j] + part[j]
        if Z <= 8:
            for k in range(Z - 1):
                resid = resid + d_recv[j, (z + 1 + k) % Z].astype(F32)
        else:
            resid = lax.fori_loop(
                0, Z - 1, lambda k, t: t + d_recv[j, (z + 1 + k) % Z].astype(F32), resid
            )
        encoded = norm_rows(resid, gain, width)
        for p in range(n):
            e_send[p, j * r:(j + 1) * r] = encoded[:, p * feat:(p + 1) * feat]
        score = score + jnp.sum(encoded.astype(F32) * weight)
    s_send[...] = jnp.full(s_send.shape, score / seq, F32)

    def e_copies(j):
        p = (me + 1 + j) % n
        return (
            remote(e_send.at[p], e_recv.at[me], e_ss.at[p], e_rs.at[me], mp=p),
            remote(s_send, s_recv.at[me], s_ss.at[p], s_rs.at[me], mp=p),
        )

    def e_start(j):
        for copy in e_copies(j):
            copy.start()

    each(n - 1, e_start)
    e_recv[me] = e_send[me]
    s_recv[me] = s_send[...]

    def e_in(j):
        src = (me + n - 1 - j) % n
        remote(e_send.at[me], e_recv.at[src], e_ss.at[me], e_rs.at[src], mp=me).wait_recv()
        remote(s_send, s_recv.at[src], s_ss.at[me], s_rs.at[src], mp=me).wait_recv()

    each(n - 1, e_in)
    per = n // triples
    lane = lax.broadcasted_iota(jnp.int32, (1, triples), 1)
    scores = jnp.zeros((1, triples), F32)
    grad = jnp.zeros((1, feat), F32)
    for t in range(triples):
        logit = s_recv[t * per]
        block = jnp.sum(e_recv[t * per].astype(F32), axis=0, keepdims=True)
        for p in range(t * per + 1, (t + 1) * per):
            logit = logit + s_recv[p]
            block = block + jnp.sum(e_recv[p].astype(F32), axis=0, keepdims=True)
        scores = jnp.where(lane == t, logit[0:1, :triples], scores)
        diff = jax.nn.sigmoid(logit[0:1, :feat]) - labels[t].astype(F32)
        grad = grad + diff * (block / seq)
    q_send[...] = grad

    def q_copy(j):
        return remote(
            q_send, q_recv.at[dme], q_ss.at[j], q_rs.at[dme], dp=(dme + j) % ndp
        )

    for j in range(1, ndp):
        q_copy(j).start()
    score_out[...] = scores
    enc_out[...] = e_recv[...]

    for j in range(chunks):
        a_copy(j).wait_send()
        sweep(first, j).wait_send()
        each(Z - 1, lambda k: d_copy(j, (z + 1 + k) % Z).wait_send())

        @pl.when(inner)
        def _():
            sweep(second, j).wait_send()

    for i in range(2):
        wx_copy(i).wait_send()
        wy_copy(i, dme).wait_send()
        wc_copy(i, dme, 0).wait_send()
        wc_copy(i, across, 1).wait_send()

    def ends(j):
        for copy in w_copies(j) + e_copies(j):
            copy.wait_send()

    each(n - 1, ends)
    for j in range(1, ndp):
        src = (dme + ndp - j) % ndp
        remote(q_send, q_recv.at[src], q_ss.at[j], q_rs.at[src], dp=dme).wait_recv()
        grad = grad + q_recv[src]
        q_copy(j).wait_send()
    grad_out[...] = grad


def on_device(
    n, ndp, table, triples, words, labels, in_gain, up_weight, down_weight, out_gain, class_weight
):
    ids = jnp.concatenate([triples, words], axis=1)
    seq = ids.shape[1]
    rows = ids.size
    tok = rows // n
    entries, width = table.shape
    units = up_weight.shape[1]
    feat = width // n
    Z = n // 2
    T = triples.shape[0]
    dma = pltpu.SemaphoreType.DMA
    vm = pl.BlockSpec(memory_space=pltpu.VMEM)
    hbm = pl.BlockSpec(memory_space=pl.ANY)
    r = min(tok, 16)
    CH = tok // r
    CR = Z * r
    ids = ids.reshape(Z, 2, CH, r).transpose(1, 2, 0, 3).reshape(2, Z * tok, 1)
    blk = pltpu.VMEM((CH, CR, width), BF16)
    wide = max(128, feat)
    enc, scores, grad = pl.pallas_call(
        functools.partial(kernel, n, ndp, seq),
        out_shape=(
            jax.ShapeDtypeStruct((n, tok, feat), BF16),
            jax.ShapeDtypeStruct((1, T), F32),
            jax.ShapeDtypeStruct((1, feat), F32),
        ),
        in_specs=[vm, hbm, hbm, hbm, vm, vm, vm, pl.BlockSpec(memory_space=pltpu.SMEM)],
        out_specs=(vm, vm, vm),
        scratch_shapes=[
            pltpu.VMEM((entries, width), BF16),
            pltpu.VMEM((width, units), BF16),
            pltpu.VMEM((units, width), BF16),
            pltpu.VMEM((width, units), BF16),
            pltpu.VMEM((units, width), BF16),
            blk, blk, blk,
            pltpu.VMEM((2, CH, CR, width), BF16),
            pltpu.VMEM((2, CH, CR, width), BF16),
            pltpu.VMEM((Z, r, width), BF16),
            pltpu.VMEM((Z, r, width), F32),
            pltpu.VMEM((CH, r, width), F32),
            pltpu.VMEM((CH, r, width), F32),
            pltpu.VMEM((CH, Z, r, width), BF16),
            pltpu.VMEM((CH, Z, r, width), BF16),
            pltpu.VMEM((n, 1, feat), F32),
            pltpu.VMEM((n, 1, feat), F32),
            pltpu.VMEM((n, tok, feat), BF16),
            pltpu.VMEM((n, tok, feat), BF16),
            pltpu.VMEM((8, wide), F32),
            pltpu.VMEM((n, 8, wide), F32),
            pltpu.VMEM((1, feat), F32),
            pltpu.VMEM((ndp, 1, feat), F32),
            dma((3,)),
            dma((2,)), dma((2,)), dma((2,)), dma((2,)), dma((2, 2)), dma((2, 2)),
            dma((CH,)), dma((CH,)), dma((2, CH)), dma((2, CH)), dma((CH, Z)), dma((CH, Z)),
            dma((2, n)), dma((2, n)),
            dma((n,)), dma((n,)), dma((n,)), dma((n,)),
            dma((ndp,)), dma((ndp,)),
        ],
        compiler_params=pltpu.CompilerParams(
            collective_id=0, has_side_effects=True, vmem_limit_bytes=63 * 1024 * 1024
        ),
    )(
        ids, table, up_weight, down_weight, in_gain.reshape(1, -1),
        out_gain.reshape(1, -1), class_weight.reshape(1, -1), labels,
    )
    return enc.reshape(rows, feat), scores.reshape(-1), grad.reshape(-1)


def solution(mesh):
    return jax.shard_map(
        functools.partial(on_device, mesh.shape["mp"], mesh.shape["dp"]),
        mesh=mesh,
        in_specs=(
            P("mp", None), P("dp", None), P("dp", None), P("dp"), P(),
            P(None, "mp"), P("mp", None), P("mp"), P("mp"),
        ),
        out_specs=(P("dp", "mp"), P("dp"), P("mp")),
        check_vma=False,
    )
```

```python
import functools
import math

import jax
import jax.numpy as jnp
from jax import lax
from jax.experimental import pallas as pl
from jax.experimental.pallas import tpu as pltpu
from jax.sharding import PartitionSpec as P

MESH = pl.DeviceIdType.MESH
BF16 = jnp.bfloat16
F32 = jnp.float32


def each(count, body):
    if count <= 8:
        for k in range(count):
            body(k)
    else:
        lax.fori_loop(0, count, lambda k, c: (body(k), c)[1], 0)


def norm_rows(values, gain, width):
    mean = jnp.sum(values, axis=1, keepdims=True) / width
    var = jnp.sum(values * values, axis=1, keepdims=True) / width - mean * mean
    return ((values - mean) * lax.rsqrt(var + 1e-05) * gain).astype(BF16)


def kernel(
    n, ndp, seq,
    ids, table, up, down, in_gain, out_gain, class_w, labels,
    enc_out, score_out, grad_out,
    tab_v, up_v, down_v, upx_v, downx_v, a_send, a_recv, own, sw_send, sw_recv,
    rows_v, terms_v, keep, part, d_send, d_recv,
    og_all, cw_all, e_send, e_recv, s_send, s_recv, q_send, q_recv,
    loc_sem, wx_ss, wx_rs, wy_ss, wy_rs, wc_ss, wc_rs, a_ss, a_rs, sw_ss, sw_rs, d_ss, d_rs,
    w_ss, w_rs, e_ss, e_rs, s_ss, s_rs, q_ss, q_rs,
):
    Z = n // 2
    me = lax.axis_index("mp")
    dme = lax.axis_index("dp")
    z, x = me // 2, me % 2
    ox = 1 - x
    partner = z * 2 + ox
    across = (dme + ndp // 2) % ndp
    beside = dme // 2 * 2 + 1 - dme % 2
    chunks, chunk_rows, width = own.shape
    r = chunk_rows // Z
    entries = table.shape[0]
    units = up.shape[1]
    feat = enc_out.shape[2]
    triples = labels.shape[0]

    def remote(src, dst, ss, rs, mp=None, dp=None):
        where = {"mp": mp} if dp is None else {"dp": dp}
        return pltpu.make_async_remote_copy(
            src_ref=src, dst_ref=dst, send_sem=ss, recv_sem=rs, device_id=where, device_id_type=MESH
        )

    loads = [
        pltpu.make_async_copy(src, dst, loc_sem.at[i])
        for i, (src, dst) in enumerate(((table, tab_v), (up, up_v), (down, down_v)))
    ]
    for copy in loads:
        copy.start()

    barrier = pltpu.get_barrier_semaphore()

    def greet(j):
        pl.semaphore_signal(barrier, inc=1, device_id={"mp": (me + 1 + j) % n}, device_id_type=MESH)

    each(n - 1, greet)
    for j in range(1, ndp):
        pl.semaphore_signal(barrier, inc=1, device_id={"dp": (dme + j) % ndp}, device_id_type=MESH)
    pl.semaphore_wait(barrier, n - 1 + ndp - 1)

    def quarter(ref, d):
        size = ref.shape[0] // ndp
        return ref.at[pl.ds(pl.multiple_of(d * size, size), size)]

    pairs = ((up, upx_v), (down, downx_v))

    def wx_copy(i):
        src, dst = pairs[i]
        return remote(quarter(src, dme), quarter(dst, dme), wx_ss.at[i], wx_rs.at[i], mp=partner)

    def wy_copy(i, d):
        ref = pairs[i][1]
        return remote(quarter(ref, d), quarter(ref, d), wy_ss.at[i], wy_rs.at[i], dp=across)

    def wc_copy(i, d, k):
        ref = pairs[i][1]
        return remote(quarter(ref, d), quarter(ref, d), wc_ss.at[i, k], wc_rs.at[i, k], dp=beside)


    def w_copies(j):
        p = (me + 1 + j) % n
        return (
            remote(out_gain, og_all.at[me], w_ss.at[0, p], w_rs.at[0, me], mp=p),
            remote(class_w, cw_all.at[me], w_ss.at[1, p], w_rs.at[1, me], mp=p),
        )

    def w_start(j):
        for copy in w_copies(j):
            copy.start()

    each(n - 1, w_start)
    og_all[me] = out_gain[...]
    cw_all[me] = class_w[...]
    loads[0].wait()

    def half(side):
        local = ids[side] - me * entries
        lanes = lax.broadcasted_iota(jnp.int32, (local.shape[0], entries), 1)
        hot = jnp.where(lanes == local, 1.0, 0.0).astype(BF16)
        embed = jnp.dot(hot, tab_v[...], preferred_element_type=F32)
        return norm_rows(embed, in_gain[...], width)

    def a_copy(j):
        return remote(a_send.at[j], a_recv.at[j], a_ss.at[j], a_rs.at[j], mp=partner)

    rows = half(ox)
    for j in range(chunks):
        a_send[j] = rows[j * chunk_rows:(j + 1) * chunk_rows]
        a_copy(j).start()
    wx_copy(0).start()
    wx_copy(1).start()
    rows = half(x)
    for j in range(chunks):
        own[j] = rows[j * chunk_rows:(j + 1) * chunk_rows]


    first = z // (Z // 2)
    second = 1 - first
    edge = jnp.logical_or(z == 0, z == Z - 1)
    inner = jnp.logical_not(edge)

    def sweep(way, j):
        return remote(
            sw_send.at[way, j], sw_recv.at[way, j], sw_ss.at[way, j], sw_rs.at[way, j],
            mp=(z + 1 - 2 * way) * 2 + x,
        )

    def sweep_in(way, j):
        return remote(
            sw_send.at[way, j], sw_recv.at[way, j], sw_ss.at[way, j], sw_rs.at[way, j], mp=me
        )

    def arrive(j):
        a_copy(j).wait_recv()
        own[j] = own[j] + a_recv[j]

        @pl.when(edge)
        def _():
            sw_recv[first, j] = jnp.zeros((chunk_rows, width), BF16)

        @pl.when(inner)
        def _():
            sweep_in(first, j).wait_recv()

        sw_send[first, j] = own[j] + sw_recv[first, j]
        sweep(first, j).start()

    def d_copy(j, zk):
        return remote(
            d_send.at[j, zk], d_recv.at[j, z], d_ss.at[j, zk], d_rs.at[j, z], mp=zk * 2 + x
        )

    def act(hidden):
        return (0.5 * hidden * (1.0 + lax.erf(hidden * (1.0 / math.sqrt(2.0))))).astype(BF16)

    def pass_back(j):
        sweep_in(second, j).wait_recv()

        @pl.when(inner)
        def _():
            sw_send[second, j] = own[j] + sw_recv[second, j]
            sweep(second, j).start()

    def finish(j):
        full = own[j] + sw_recv[0, j] + sw_recv[1, j]
        for zk in range(Z):
            rows_v[zk] = full[zk * r:(zk + 1) * r]
        keep[j] = rows_v[z].astype(F32)
        mine = act(jnp.dot(full, up_v[...], preferred_element_type=F32))
        theirs = act(jnp.dot(full, upx_v[...], preferred_element_type=F32))
        terms = jnp.dot(mine, down_v[...], preferred_element_type=F32)
        terms = terms + jnp.dot(theirs, downx_v[...], preferred_element_type=F32)
        for zk in range(Z):
            terms_v[zk] = terms[zk * r:(zk + 1) * r]
            d_send[j, zk] = terms[zk * r:(zk + 1) * r].astype(BF16)
        each(Z - 1, lambda k: d_copy(j, (z + 1 + k) % Z).start())
        part[j] = terms_v[z]

    def relay(i):
        wx_copy(i).wait_recv()
        wy_copy(i, dme).start()
        wc_copy(i, dme, 0).start()

    def relay_on(i):
        wy_copy(i, across).wait_recv()
        wc_copy(i, across, 1).start()

    early, lag = 0, min(2, chunks)
    for i in range(early):
        relay(i)
    for t in range(chunks + lag):
        if t < chunks:
            arrive(t)
        if t == 0:
            for i in range(early):
                relay_on(i)
        if t == chunks - 1:
            for i in range(early, 2):
                relay(i)
        if t >= lag:
            pass_back(t - lag)
    for i in range(early, 2):
        relay_on(i)
    for i in range(2):
        wc_copy(i, beside, 0).wait_recv()
        wc_copy(i, (beside + ndp // 2) % ndp, 1).wait_recv()
    loads[1].wait()
    loads[2].wait()
    for j in range(chunks):
        finish(j)

    def w_in(j):
        src = (me + n - 1 - j) % n
        for i, (ref, dst) in enumerate(((out_gain, og_all), (class_w, cw_all))):
            remote(ref, dst.at[src], w_ss.at[i, me], w_rs.at[i, src], mp=me).wait_recv()

    each(n - 1, w_in)
    gain = jnp.concatenate([og_all[p] for p in range(n)], axis=1)
    weight = jnp.concatenate([cw_all[p] for p in range(n)], axis=1)

    def d_in(j, zs):
        return remote(d_send.at[j, z], d_recv.at[j, zs], d_ss.at[j, z], d_rs.at[j, zs], mp=me)

    score = jnp.zeros((), F32)
    for j in range(chunks):
        each(Z - 1, lambda k: d_in(j, (z + 1 + k) % Z).wait_recv())
        resid = keep[j] + part[j]
        if Z <= 8:
            for k in range(Z - 1):
                resid = resid + d_recv[j, (z + 1 + k) % Z].astype(F32)
        else:
            resid = lax.fori_loop(
                0, Z - 1, lambda k, t: t + d_recv[j, (z + 1 + k) % Z].astype(F32), resid
            )
        encoded = norm_rows(resid, gain, width)
        for p in range(n):
            e_send[p, j * r:(j + 1) * r] = encoded[:, p * feat:(p + 1) * feat]
        score = score + jnp.sum(encoded.astype(F32) * weight)
    s_send[...] = jnp.full(s_send.shape, score / seq, F32)

    def e_copies(j):
        p = (me + 1 + j) % n
        return (
            remote(e_send.at[p], e_recv.at[me], e_ss.at[p], e_rs.at[me], mp=p),
            remote(s_send, s_recv.at[me], s_ss.at[p], s_rs.at[me], mp=p),
        )

    def e_start(j):
        for copy in e_copies(j):
            copy.start()

    each(n - 1, e_start)
    e_recv[me] = e_send[me]
    s_recv[me] = s_send[...]

    def e_in(j):
        src = (me + n - 1 - j) % n
        remote(e_send.at[me], e_recv.at[src], e_ss.at[me], e_rs.at[src], mp=me).wait_recv()
        remote(s_send, s_recv.at[src], s_ss.at[me], s_rs.at[src], mp=me).wait_recv()

    each(n - 1, e_in)
    per = n // triples
    lane = lax.broadcasted_iota(jnp.int32, (1, triples), 1)
    scores = jnp.zeros((1, triples), F32)
    grad = jnp.zeros((1, feat), F32)
    for t in range(triples):
        logit = s_recv[t * per]
        block = jnp.sum(e_recv[t * per].astype(F32), axis=0, keepdims=True)
        for p in range(t * per + 1, (t + 1) * per):
            logit = logit + s_recv[p]
            block = block + jnp.sum(e_recv[p].astype(F32), axis=0, keepdims=True)
        scores = jnp.where(lane == t, logit[0:1, :triples], scores)
        diff = jax.nn.sigmoid(logit[0:1, :feat]) - labels[t].astype(F32)
        grad = grad + diff * (block / seq)
    q_send[...] = grad

    def q_copy(j):
        return remote(
            q_send, q_recv.at[dme], q_ss.at[j], q_rs.at[dme], dp=(dme + j) % ndp
        )

    for j in range(1, ndp):
        q_copy(j).start()
    score_out[...] = scores
    enc_out[...] = e_recv[...]

    for j in range(chunks):
        a_copy(j).wait_send()
        sweep(first, j).wait_send()
        each(Z - 1, lambda k: d_copy(j, (z + 1 + k) % Z).wait_send())

        @pl.when(inner)
        def _():
            sweep(second, j).wait_send()

    for i in range(2):
        wx_copy(i).wait_send()
        wy_copy(i, dme).wait_send()
        wc_copy(i, dme, 0).wait_send()
        wc_copy(i, across, 1).wait_send()

    def ends(j):
        for copy in w_copies(j) + e_copies(j):
            copy.wait_send()

    each(n - 1, ends)
    for j in range(1, ndp):
        src = (dme + ndp - j) % ndp
        remote(q_send, q_recv.at[src], q_ss.at[j], q_rs.at[src], dp=dme).wait_recv()
        grad = grad + q_recv[src]
        q_copy(j).wait_send()
    grad_out[...] = grad


def on_device(
    n, ndp, table, triples, words, labels, in_gain, up_weight, down_weight, out_gain, class_weight
):
    ids = jnp.concatenate([triples, words], axis=1)
    seq = ids.shape[1]
    rows = ids.size
    tok = rows // n
    entries, width = table.shape
    units = up_weight.shape[1]
    feat = width // n
    Z = n // 2
    T = triples.shape[0]
    dma = pltpu.SemaphoreType.DMA
    vm = pl.BlockSpec(memory_space=pltpu.VMEM)
    hbm = pl.BlockSpec(memory_space=pl.ANY)
    r = min(tok, 16)
    CH = tok // r
    CR = Z * r
    ids = ids.reshape(Z, 2, CH, r).transpose(1, 2, 0, 3).reshape(2, Z * tok, 1)
    blk = pltpu.VMEM((CH, CR, width), BF16)
    wide = max(128, feat)
    enc, scores, grad = pl.pallas_call(
        functools.partial(kernel, n, ndp, seq),
        out_shape=(
            jax.ShapeDtypeStruct((n, tok, feat), BF16),
            jax.ShapeDtypeStruct((1, T), F32),
            jax.ShapeDtypeStruct((1, feat), F32),
        ),
        in_specs=[vm, hbm, hbm, hbm, vm, vm, vm, pl.BlockSpec(memory_space=pltpu.SMEM)],
        out_specs=(vm, vm, vm),
        scratch_shapes=[
            pltpu.VMEM((entries, width), BF16),
            pltpu.VMEM((width, units), BF16),
            pltpu.VMEM((units, width), BF16),
            pltpu.VMEM((width, units), BF16),
            pltpu.VMEM((units, width), BF16),
            blk, blk, blk,
            pltpu.VMEM((2, CH, CR, width), BF16),
            pltpu.VMEM((2, CH, CR, width), BF16),
            pltpu.VMEM((Z, r, width), BF16),
            pltpu.VMEM((Z, r, width), F32),
            pltpu.VMEM((CH, r, width), F32),
            pltpu.VMEM((CH, r, width), F32),
            pltpu.VMEM((CH, Z, r, width), BF16),
            pltpu.VMEM((CH, Z, r, width), BF16),
            pltpu.VMEM((n, 1, feat), F32),
            pltpu.VMEM((n, 1, feat), F32),
            pltpu.VMEM((n, tok, feat), BF16),
            pltpu.VMEM((n, tok, feat), BF16),
            pltpu.VMEM((8, wide), F32),
            pltpu.VMEM((n, 8, wide), F32),
            pltpu.VMEM((1, feat), F32),
            pltpu.VMEM((ndp, 1, feat), F32),
            dma((3,)),
            dma((2,)), dma((2,)), dma((2,)), dma((2,)), dma((2, 2)), dma((2, 2)),
            dma((CH,)), dma((CH,)), dma((2, CH)), dma((2, CH)), dma((CH, Z)), dma((CH, Z)),
            dma((2, n)), dma((2, n)),
            dma((n,)), dma((n,)), dma((n,)), dma((n,)),
            dma((ndp,)), dma((ndp,)),
        ],
        compiler_params=pltpu.CompilerParams(
            collective_id=0, has_side_effects=True, vmem_limit_bytes=63 * 1024 * 1024
        ),
    )(
        ids, table, up_weight, down_weight, in_gain.reshape(1, -1),
        out_gain.reshape(1, -1), class_weight.reshape(1, -1), labels,
    )
    return enc.reshape(rows, feat), scores.reshape(-1), grad.reshape(-1)


def solution(mesh):
    return jax.shard_map(
        functools.partial(on_device, mesh.shape["mp"], mesh.shape["dp"]),
        mesh=mesh,
        in_specs=(
            P("mp", None), P("dp", None), P("dp", None), P("dp"), P(),
            P(None, "mp"), P("mp", None), P("mp"), P("mp"),
        ),
        out_specs=(P("dp", "mp"), P("dp"), P("mp")),
        check_vma=False,
    )
```
